32 devices in a mesh: blk: 8 (over y, x, core), vec: 4 (over z).
Axes of the slice: x: 2, y: 2, z: 4, core: 2. Of those that a mesh axis runs over, the one named last changes fastest.
Arguments:
- trial: bfloat16 [64, 64, 4096], P('vec', None, 'blk'), may hold values from -0.01171875 to 0.01171875
- coupling: bfloat16 [8, 6, 512, 512], P('blk'), may hold values from -0.09375 to 0.09375
- partners: int32 [8, 6], P('blk'), may hold values from 0 to 7, as said below
- live: int32 [8], P('blk'), may hold values from 1 to 6, as said below
- diag_block: bfloat16 [4096, 512], P('blk'), may hold values from -0.25 to 0.25
- beta_coupling: bfloat16 [64, 64], replicated, may hold values from -0.75 to 0.75
- hdiag: float32 [64, 4096], P(None, 'blk'), may hold values from 0.5 to 4
Outputs:
- correction: bfloat16 [64, 64, 4096], P('vec', None, 'blk')
- subspace: float32 [64, 64], P(None, 'vec')
The draws below stay inside these ranges and needn't reach their ends.
Inputs may be any that keep to these rules, and one draw needn't show every extreme that they name: `partners`: each row holds 6 different block numbers, none equal to the row's own block. `live`: some block uses all 6 slots in every draw.
All inputs are finite; a program needn't handle non-finite values.
Results may differ from the reference program's by a relative error of at most 0.0012.
Values may be sent and summed in bfloat16 or wider, within the bound.
A program may use at most 128 MiB of HBM per device.

```python
import jax
import jax.numpy as jnp
from jax import lax

K = 64
A_BLK = 512
NBETA = 64
COUP = 6
NBLOCKS = 8
NA = 4096


def draw_partners(key, part):
    nblocks = NA // A_BLK
    keys = jax.random.split(jax.random.fold_in(key, 11), nblocks)

    def one_row(row_key, position):
        order = jax.random.permutation(row_key, nblocks - 1)[:COUP]
        return ((position + 1 + order) % nblocks).astype(jnp.int32)
    return jax.vmap(one_row)(keys, jnp.arange(nblocks, dtype=jnp.int32))


def draw_live(key, part):
    nblocks = NA // A_BLK
    counts = jax.random.randint(jax.random.fold_in(key, 23), (nblocks,), 1, COUP + 1)
    chosen = jax.random.randint(jax.random.fold_in(key, 29), (), 0, nblocks)
    return jnp.where(jnp.arange(nblocks, dtype=jnp.int32) == chosen, COUP, counts).astype(jnp.int32)


def levels(key, shape, shards, least, largest):
    factor_of, own = 1.0, jax.random.fold_in(key, 6)
    for dim, shards_of in shards:
        heights = jnp.exp(jax.random.uniform(jax.random.fold_in(own, dim), (shards_of,), jnp.float32, least / len(shards), largest / len(shards)))
        factor_of = factor_of * jnp.repeat(heights, shape[dim] // shards_of).reshape([-1 if axis == dim else 1 for axis in range(len(shape))])
    return factor_of


def centred(rng, shape, width, bound, pieces=(), kind=jnp.bfloat16):
    result = jax.random.normal(rng, shape, jnp.float32) * width
    if len(pieces) > 0:
        result = levels(rng, shape, pieces, -0.22, 0.18) * result
    return jnp.clip(result, min=-bound, max=bound).astype(kind)


def setup_inputs(seed: int = 0) -> dict:
    splits = jax.random.split(jax.random.key(seed), 8)
    trial = centred(splits[0], (K, NBETA, NA), (1.0 / (NA * NBETA) ** 0.5), 0.01171875, ((0, 4), (2, 8)))
    coupling = centred(splits[1], (NBLOCKS, COUP, A_BLK, A_BLK), (A_BLK * (COUP + 2)) ** -0.5, 0.09375, ((0, 8),))
    partners = draw_partners(jax.random.fold_in(splits[7], 71), 0)
    live = draw_live(jax.random.fold_in(splits[7], 71), 0)
    diag_block = centred(splits[4], (NA, A_BLK), A_BLK ** -0.5, 0.25, ((0, 8),))
    beta_coupling = centred(splits[5], (NBETA, NBETA), NBETA ** -0.5, 0.75)
    hdiag = jnp.clip(0.5 + 3.5 * jax.random.uniform(splits[6], (NBETA, NA), jnp.float32) ** levels(splits[6], (NBETA, NA), ((1, 8),), -0.2, 0.2), 0.5, 4.0)
    return dict(trial=trial, coupling=coupling, partners=partners, live=live, diag_block=diag_block, beta_coupling=beta_coupling, hdiag=hdiag)


def reference(trial, coupling, partners, live, diag_block, beta_coupling, hdiag):
    nblocks = NA // A_BLK
    row_count = K * NBETA
    flat = trial.reshape(row_count, NA)
    diag_three = diag_block.reshape(nblocks, A_BLK, A_BLK)
    contract = (((1,), (1,)), ((), ()))

    def one_block(entries):
        blocks, partner_ids, live_count, own_block, position = entries
        own_rows = lax.dynamic_slice_in_dim(flat, position * A_BLK, A_BLK, 1)
        running = lax.dot_general(own_rows, own_block, contract, preferred_element_type=jnp.float32)
        for member in range(COUP):
            segment = lax.dynamic_slice_in_dim(flat, (partner_ids[member] * A_BLK).astype(jnp.int32), A_BLK, 1)
            term = lax.dot_general(segment, blocks[member], contract, preferred_element_type=jnp.float32)
            running = running + jnp.where(member < live_count, term, jnp.float32(0.0))
        return running
    stacked = lax.map(one_block, (coupling, partners, live, diag_three, jnp.arange(nblocks, dtype=jnp.int32)))
    alpha_part = jnp.transpose(stacked, (1, 0, 2)).reshape(K, NBETA, NA)
    trial_float = trial.astype(jnp.float32)
    beta_part = jnp.einsum('bc,kca->kba', beta_coupling.astype(jnp.float32), trial_float)
    sigma = alpha_part + beta_part + hdiag[None] * trial_float
    subspace = jnp.einsum('kba,lba->kl', trial_float, sigma, precision=lax.Precision.HIGHEST)
    theta = jnp.diagonal(subspace)
    resid = sigma - theta[:, None, None] * trial_float
    gap = theta[:, None, None] - hdiag[None]
    raw = resid * gap / (gap * gap + 0.25)
    msq = lax.optimization_barrier(jnp.mean(raw * raw, axis=(1, 2)))
    correction = (raw * lax.rsqrt(msq + 1e-06)[:, None, None]).astype(jnp.bfloat16)
    return (correction, subspace)
```

```python
import functools

import jax
import jax.numpy as jnp
from jax import lax
from jax.experimental import pallas as pl
from jax.experimental.pallas import tpu as pltpu
from jax.sharding import PartitionSpec as P


def gathered(trial, coupling, partners, live, diag_block, beta_coupling, hdiag):
    root_count, beta_count, block_width = trial.shape
    row_count = root_count * beta_count
    contract = (((1,), (1,)), ((), ()))
    blocks = coupling[0]
    partner_ids = partners[0]
    live_count = live[0]
    flat = trial.reshape(row_count, block_width)
    sigma_flat = lax.dot_general(flat, diag_block, contract, preferred_element_type=jnp.float32)
    empty = jnp.zeros((row_count, block_width), jnp.float32)
    running = empty
    segment = lax.all_gather(trial, "blk", axis=2, tiled=True)
    span_width = segment.shape[2]
    seg_flat = segment.reshape(row_count, span_width)
    for member in range(blocks.shape[0]):
        relative = partner_ids[member] * block_width
        inside = (relative >= 0) & (relative + block_width <= span_width) & (member < live_count)
        start = jnp.clip(relative, 0, span_width - block_width)

        def multiply(total, start=start, member=member):
            piece = lax.dynamic_slice_in_dim(seg_flat, start, block_width, 1)
            return total + lax.dot_general(
                piece, blocks[member], contract, preferred_element_type=jnp.float32
            )

        def unchanged(total):
            return total

        running = lax.cond(inside, multiply, unchanged, running)
    trial_float = trial.astype(jnp.float32)
    beta_part = jnp.einsum("bc,kca->kba", beta_coupling, trial, preferred_element_type=jnp.float32)
    sigma = (
        (sigma_flat + running).reshape(root_count, beta_count, block_width)
        + beta_part
        + hdiag[None] * trial_float
    )
    all_roots = lax.all_gather(trial, "vec", axis=0, tiled=True)
    intersection_part = jnp.einsum(
        "kba,lba->kl", all_roots.astype(jnp.float32), sigma, precision=lax.Precision.HIGHEST
    )
    total_cells = beta_count * block_width * lax.axis_size("blk")
    theta_part = jnp.einsum("kba,kba->k", trial_float, sigma, precision=lax.Precision.HIGHEST)
    theta = lax.psum(theta_part, "blk")
    resid = sigma - theta[:, None, None] * trial_float
    gap = theta[:, None, None] - hdiag[None]
    raw = resid * gap / (gap * gap + 0.25)
    squares, subspace = lax.psum((jnp.sum(raw * raw, axis=(1, 2)), intersection_part), "blk")
    msq = squares / total_cells
    correction = (raw * lax.rsqrt(msq + 1e-06)[:, None, None]).astype(jnp.bfloat16)
    return (correction, subspace)


CHUNKS = 4
MESH = pl.DeviceIdType.MESH
CONTRACT = (((1,), (1,)), ((), ()))


def kernel(
    depth, partners, live, trial, coupling, diag, beta, hdiag, correction, subspace,
    held, weights, slots, roots, sigma, rounded, edge, rows, stats, products, theta, totals, edge_total,
    load_sem, blk_send, blk_recv, vec_send, vec_recv, stat_send, stat_recv, edge_send, edge_recv,
):
    me, z = lax.axis_index("blk"), lax.axis_index("vec")
    root_count, beta_count, width = trial.shape
    piece = beta_count // CHUNKS
    cells = root_count * piece
    last = CHUNKS - 1
    members = held.shape[0]
    core, x, y = me % 2, (me // 2) % 2, me // 4
    is_end = (z == 0) | (z == depth - 1)
    mate = z + 1 - 2 * (z % 2)

    def peer(r):
        flip = lambda bit, on: 1 - bit if on else bit
        return flip(y, r & 4) * 4 + flip(x, r & 2) * 2 + flip(core, r & 1)

    def part(ref, c):
        return ref.at[:, pl.ds(c * piece, piece), :]

    def remote(src, dst, send, recv, device):
        return pltpu.make_async_remote_copy(
            src_ref=src, dst_ref=dst, send_sem=send, recv_sem=recv, device_id=device, device_id_type=MESH
        )

    loads = [
        pltpu.make_async_copy(trial, held.at[0], load_sem.at[0]),
        pltpu.make_async_copy(diag, weights.at[0], load_sem.at[1]),
        pltpu.make_async_copy(coupling.at[0], slots, load_sem.at[2]),
        pltpu.make_async_copy(trial, roots.at[z], load_sem.at[3]),
    ]
    for load in loads:
        load.start()

    barrier = pltpu.get_barrier_semaphore()
    for r in range(1, members):
        pl.semaphore_signal(barrier, inc=1, device_id={"blk": peer(r)}, device_id_type=MESH)

    @pl.when(z < depth - 1)
    def _():
        pl.semaphore_signal(barrier, inc=1, device_id={"vec": z + 1}, device_id_type=MESH)

    @pl.when(z > 0)
    def _():
        pl.semaphore_signal(barrier, inc=1, device_id={"vec": z - 1}, device_id_type=MESH)

    pl.semaphore_wait(barrier, members + 1 - is_end.astype(jnp.int32))

    def blk_copy(r, hop, c):
        src = trial if r == 0 else held.at[r]
        return remote(
            part(src, c), part(held.at[r ^ hop], c), blk_send.at[r ^ hop, c], blk_recv.at[r ^ hop, c],
            {"blk": peer(hop)},
        )

    sent = []

    def blk_start(r, hop, c):
        copy = blk_copy(r, hop, c)
        copy.start()
        sent.append(copy)

    def blk_wait(slot, c):
        blk_copy(0, slot, c).wait_recv()

    def vec_copy(origin, side, c, src):
        return remote(
            part(src, c), part(roots.at[origin], c), vec_send.at[side, origin, c], vec_recv.at[origin, c],
            {"vec": z + 1 - 2 * side},
        )

    def goes(side, c):
        limit = 2 if c == last else 1
        return (z < depth - limit) if side == 0 else (z >= limit)

    def has(step, side, c):
        origin = z - step if side == 0 else z + step
        there = (origin >= 0) & (origin < depth)
        if c == last:
            there = there & jnp.logical_not(is_end)
        return there, origin

    for c in range(CHUNKS):
        blk_start(0, 2, c)
        blk_start(0, 4, (c + 2) % CHUNKS)
        blk_start(0, 1, c)
        for side in (0, 1):
            @pl.when(goes(side, c))
            def _():
                vec_copy(z, side, c, trial).start()

    def vec_step(step, c):
        for side in (0, 1):
            there, origin = has(step, side, c)

            @pl.when(there)
            def _():
                vec_copy(origin, side, c, trial).wait_recv()

            @pl.when(there & goes(side, c))
            def _():
                vec_copy(origin, side, c, roots.at[origin]).start()

    for load in loads:
        load.wait()

    def select(r):
        block = peer(r)
        index, hit = jnp.int32(0), jnp.float32(0.0)
        for c in range(slots.shape[0]):
            match = (partners[0, c] == block) & (c < live[0])
            index = jnp.where(match, c, index)
            hit = jnp.where(match, jnp.float32(1.0), hit)
        weights[r] = (slots[index].astype(jnp.float32) * hit).astype(weights.dtype)

    for r in range(1, members):
        select(r)

    def own(k, _):
        vectors = held[0, k]
        sigma[k] = (
            jnp.dot(beta[...], vectors, preferred_element_type=jnp.float32)
            + hdiag[...] * vectors.astype(jnp.float32)
        )
        return 0

    lax.fori_loop(0, root_count, own, 0)

    def multiply(r, c):
        span = pl.ds(pl.multiple_of(c * piece, piece), piece)
        left = held[r, :, span, :].reshape(cells, width)
        out = lax.dot_general(left, weights[r], CONTRACT, preferred_element_type=jnp.float32)
        sigma[:, span, :] += out.reshape(root_count, piece, width)

    def multiply_all(first, count):
        def body(i, _):
            multiply(first + i // CHUNKS, i % CHUNKS)
            return 0

        lax.fori_loop(0, count * CHUNKS, body, 0)

    for c in range(CHUNKS):
        blk_wait(1, c)
    multiply_all(0, 2)
    products[...] = jnp.zeros_like(products)

    for t in range(CHUNKS):
        u = (t + 2) % CHUNKS
        blk_wait(2, t)
        if t < 2:
            blk_start(2, 4, t)
        blk_start(2, 1, t)
        blk_wait(4, u)
        if t < 2:
            blk_start(4, 2, u)
        blk_start(4, 1, u)
        vec_step(1, t)
    for c in range(CHUNKS):
        blk_wait(3, c)
        blk_wait(5, c)
    multiply_all(2, 4)
    for t in range(2):
        for c in (t, t + 2):
            blk_wait(6, c)
            blk_start(6, 1, c)
        vec_step(2, t)
        for c in (t, t + 2):
            blk_wait(7, c)

        def tail(i, _, t=t):
            multiply(6 + i // 2, t + 2 * (i % 2))
            return 0

        lax.fori_loop(0, 4, tail, 0)

    def share(phase):
        for r in range(1, members):
            place = stats.at[phase, me]
            remote(place, place, stat_send.at[phase, r], stat_recv.at[phase, me], {"blk": peer(r)}).start()

    def gather(phase):
        for r in range(1, members):
            place = stats.at[phase, peer(r)]
            remote(place, place, stat_send.at[phase, r], stat_recv.at[phase, peer(r)], {"blk": peer(r)}).wait_recv()
        total = stats[phase, 0]
        for j in range(1, members):
            total = total + stats[phase, j]
        return total

    def finish(k, _):
        value = sigma[k]
        rounded[k] = value.astype(rounded.dtype)
        rows[pl.ds(k, 1), :] = jnp.sum(value * held[0, k].astype(jnp.float32), axis=0, keepdims=True)
        return 0

    lax.fori_loop(0, root_count, finish, 0)
    stats[0, me] = jnp.broadcast_to(jnp.sum(rows[...], axis=1, keepdims=True), stats.shape[2:])
    share(0)

    def edge_copy():
        return remote(part(rounded, last), edge, edge_send.at[0], edge_recv.at[0], {"vec": mate})

    def total_copy():
        return remote(edge_total.at[0], edge_total.at[1], edge_send.at[1], edge_recv.at[1], {"vec": mate})

    @pl.when(is_end)
    def _():
        edge_copy().start()

    row = lax.broadcasted_iota(jnp.int32, (cells, cells), 0) % piece
    column = lax.broadcasted_iota(jnp.int32, (cells, cells), 1) % piece
    same = (row == column).astype(jnp.float32)

    def product(which, origin, c, right):
        span = pl.ds(pl.multiple_of(c * piece, piece), piece)
        left = roots[origin, :, span, :].reshape(cells, width)
        out = lax.dot_general(left, right.reshape(cells, width), CONTRACT, preferred_element_type=jnp.float32)
        out = jnp.sum((out * same).reshape(root_count, piece, cells), axis=1)
        place = pl.ds(pl.multiple_of(origin * root_count, root_count), root_count)
        products[which, place, :] += out

    def products_of(origin, start, stop):
        def body(c, _):
            span = pl.ds(pl.multiple_of(c * piece, piece), piece)
            product(0, origin, c, rounded[:, span, :])
            return 0

        lax.fori_loop(start, stop, body, 0)

    def products_at(step, start, stop):
        for side in (0, 1):
            for low, high in ((start, min(stop, last)), (max(start, last), stop)):
                if low < high:
                    there, origin = has(step, side, low)

                    @pl.when(there)
                    def _():
                        products_of(origin, low, high)

    products_of(z, 0, last)

    @pl.when(jnp.logical_not(is_end))
    def _():
        products_of(z, last, CHUNKS)

    products_at(1, 0, CHUNKS)

    theta[...] = jnp.broadcast_to(gather(0)[:, :1], theta.shape)

    def residual(k, _):
        value = theta[pl.ds(k, 1), :]
        resid = sigma[k] - value * held[0, k].astype(jnp.float32)
        gap = value - hdiag[...]
        raw = resid * gap / (gap * gap + 0.25)
        sigma[k] = raw
        rows[pl.ds(k, 1), :] = jnp.sum(raw * raw, axis=0, keepdims=True)
        return 0

    lax.fori_loop(0, root_count, residual, 0)
    stats[1, me] = jnp.broadcast_to(jnp.sum(rows[...], axis=1, keepdims=True), stats.shape[2:])
    share(1)
    vec_step(2, 2)
    products_at(2, 0, last)
    msq = gather(1) / (beta_count * width * members)
    theta[...] = jnp.broadcast_to(lax.rsqrt(msq + 1e-06)[:, :1], theta.shape)

    def scale(k, _):
        correction[k] = (sigma[k] * theta[pl.ds(k, 1), :]).astype(correction.dtype)
        return 0

    lax.fori_loop(0, root_count, scale, 0)

    pick = (
        lax.broadcasted_iota(jnp.int32, (root_count, cells), 1) // piece
        == lax.broadcasted_iota(jnp.int32, (root_count, cells), 0)
    ).astype(jnp.float32)

    def collect(which):
        return lax.dot_general(
            pick, products[which], CONTRACT, precision=lax.Precision.HIGHEST, preferred_element_type=jnp.float32
        )

    vec_step(2, last)
    products_at(2, last, CHUNKS)

    @pl.when(jnp.logical_not(is_end))
    def _():
        edge_copy().wait_recv()

        def body(origin, _):
            product(1, origin, last, edge[...])
            return 0

        lax.fori_loop(0, depth, body, 0)
        edge_total[0] = collect(1)
        total_copy().start()

    for c in range(last):
        vec_step(3, c)
        products_at(3, c, c + 1)
    totals[...] = collect(0)

    @pl.when(is_end)
    def _():
        total_copy().wait_recv()
        totals[...] += edge_total[1]

    stats[2, me] = totals[...]
    share(2)

    for copy in sent:
        copy.wait_send()
    for side in (0, 1):
        for c in range(CHUNKS):
            @pl.when(goes(side, c))
            def _():
                vec_copy(z, side, c, trial).wait_send()

            for step in range(1, depth):
                there, origin = has(step, side, c)

                @pl.when(there & goes(side, c))
                def _():
                    vec_copy(origin, side, c, trial).wait_send()

    @pl.when(is_end)
    def _():
        edge_copy().wait_send()

    @pl.when(jnp.logical_not(is_end))
    def _():
        total_copy().wait_send()

    subspace[...] = gather(2)
    for phase in range(3):
        for r in range(1, members):
            place = stats.at[phase, me]
            remote(place, place, stat_send.at[phase, r], stat_recv.at[phase, me], {"blk": peer(r)}).wait_send()


def exchanged(depth, members, trial, coupling, partners, live, diag_block, beta_coupling, hdiag):
    root_count, beta_count, width = trial.shape
    slot_count = coupling.shape[1]
    cells = root_count * (beta_count // CHUNKS)
    lanes = 128
    kind, full = trial.dtype, jnp.float32
    vmem, smem, anywhere = (
        pl.BlockSpec(memory_space=pltpu.VMEM),
        pl.BlockSpec(memory_space=pltpu.SMEM),
        pl.BlockSpec(memory_space=pl.ANY),
    )
    dma = pltpu.SemaphoreType.DMA
    correction, subspace = pl.pallas_call(
        functools.partial(kernel, depth),
        out_shape=(
            jax.ShapeDtypeStruct(trial.shape, kind),
            jax.ShapeDtypeStruct((root_count, lanes), full),
        ),
        in_specs=[smem, smem, anywhere, anywhere, anywhere, vmem, vmem],
        out_specs=(vmem, vmem),
        scratch_shapes=[
            pltpu.VMEM((members,) + trial.shape, kind),
            pltpu.VMEM((members, width, width), kind),
            pltpu.VMEM((slot_count, width, width), kind),
            pltpu.VMEM((depth,) + trial.shape, kind),
            pltpu.VMEM(trial.shape, full),
            pltpu.VMEM(trial.shape, kind),
            pltpu.VMEM((root_count, beta_count // CHUNKS, width), kind),
            pltpu.VMEM((root_count, width), full),
            pltpu.VMEM((3, members, root_count, lanes), full),
            pltpu.VMEM((2, lanes, cells), full),
            pltpu.VMEM((root_count, width), full),
            pltpu.VMEM((root_count, lanes), full),
            pltpu.VMEM((2, root_count, lanes), full),
            dma((4,)),
            dma((members, CHUNKS)),
            dma((members, CHUNKS)),
            dma((2, depth, CHUNKS)),
            dma((depth, CHUNKS)),
            dma((3, members)),
            dma((3, members)),
            dma((2,)),
            dma((2,)),
        ],
        compiler_params=pltpu.CompilerParams(collective_id=0, has_side_effects=True, vmem_limit_bytes=50 * 2**20),
        name="davidson",
    )(partners, live, trial, coupling, diag_block, beta_coupling, hdiag)
    return correction, subspace[:, : root_count * depth].T


def solution(mesh):
    depth, members = mesh.shape["vec"], mesh.shape["blk"]
    if depth == 4 and members == 8:
        local = functools.partial(exchanged, depth, members)
    else:
        local = gathered
    in_specs = (
        P("vec", None, "blk"),
        P("blk", None, None, None),
        P("blk", None),
        P("blk"),
        P("blk", None),
        P(),
        P(None, "blk"),
    )
    out_specs = (P("vec", None, "blk"), P(None, "vec"))
    return jax.shard_map(local, mesh=mesh, in_specs=in_specs, out_specs=out_specs, check_vma=False)
```

```python
import functools

import jax
import jax.numpy as jnp
from jax import lax
from jax.experimental import pallas as pl
from jax.experimental.pallas import tpu as pltpu
from jax.sharding import PartitionSpec as P


def gathered(trial, coupling, partners, live, diag_block, beta_coupling, hdiag):
    root_count, beta_count, block_width = trial.shape
    row_count = root_count * beta_count
    contract = (((1,), (1,)), ((), ()))
    blocks = coupling[0]
    partner_ids = partners[0]
    live_count = live[0]
    flat = trial.reshape(row_count, block_width)
    sigma_flat = lax.dot_general(flat, diag_block, contract, preferred_element_type=jnp.float32)
    empty = jnp.zeros((row_count, block_width), jnp.float32)
    running = empty
    segment = lax.all_gather(trial, "blk", axis=2, tiled=True)
    span_width = segment.shape[2]
    seg_flat = segment.reshape(row_count, span_width)
    for member in range(blocks.shape[0]):
        relative = partner_ids[member] * block_width
        inside = (relative >= 0) & (relative + block_width <= span_width) & (member < live_count)
        start = jnp.clip(relative, 0, span_width - block_width)

        def multiply(total, start=start, member=member):
            piece = lax.dynamic_slice_in_dim(seg_flat, start, block_width, 1)
            return total + lax.dot_general(
                piece, blocks[member], contract, preferred_element_type=jnp.float32
            )

        def unchanged(total):
            return total

        running = lax.cond(inside, multiply, unchanged, running)
    trial_float = trial.astype(jnp.float32)
    beta_part = jnp.einsum("bc,kca->kba", beta_coupling, trial, preferred_element_type=jnp.float32)
    sigma = (
        (sigma_flat + running).reshape(root_count, beta_count, block_width)
        + beta_part
        + hdiag[None] * trial_float
    )
    all_roots = lax.all_gather(trial, "vec", axis=0, tiled=True)
    intersection_part = jnp.einsum(
        "kba,lba->kl", all_roots.astype(jnp.float32), sigma, precision=lax.Precision.HIGHEST
    )
    total_cells = beta_count * block_width * lax.axis_size("blk")
    theta_part = jnp.einsum("kba,kba->k", trial_float, sigma, precision=lax.Precision.HIGHEST)
    theta = lax.psum(theta_part, "blk")
    resid = sigma - theta[:, None, None] * trial_float
    gap = theta[:, None, None] - hdiag[None]
    raw = resid * gap / (gap * gap + 0.25)
    squares, subspace = lax.psum((jnp.sum(raw * raw, axis=(1, 2)), intersection_part), "blk")
    msq = squares / total_cells
    correction = (raw * lax.rsqrt(msq + 1e-06)[:, None, None]).astype(jnp.bfloat16)
    return (correction, subspace)


CHUNKS = 4
MESH = pl.DeviceIdType.MESH
CONTRACT = (((1,), (1,)), ((), ()))


def kernel(
    depth, partners_in, live, trial, coupling, diag, beta_in, hdiag_in, correction, subspace,
    partners, beta, hdiag, held, weights, slots, roots, sigma, rounded, edge, rows, stats, products, theta, totals, edge_total,
    load_sem, blk_send, blk_recv, vec_send, vec_recv, stat_send, stat_recv, edge_send, edge_recv,
):
    me, z = lax.axis_index("blk"), lax.axis_index("vec")
    root_count, beta_count, width = trial.shape
    piece = beta_count // CHUNKS
    cells = root_count * piece
    last = CHUNKS - 1
    members = held.shape[0]
    core, x, y = me % 2, (me // 2) % 2, me // 4
    is_end = (z == 0) | (z == depth - 1)
    mate = z + 1 - 2 * (z % 2)

    def peer(r):
        flip = lambda bit, on: 1 - bit if on else bit
        return flip(y, r & 4) * 4 + flip(x, r & 2) * 2 + flip(core, r & 1)

    def part(ref, c):
        return ref.at[:, pl.ds(c * piece, piece), :]

    def remote(src, dst, send, recv, device):
        return pltpu.make_async_remote_copy(
            src_ref=src, dst_ref=dst, send_sem=send, recv_sem=recv, device_id=device, device_id_type=MESH
        )

    loads = [
        pltpu.make_async_copy(trial, held.at[0], load_sem.at[0]),
        pltpu.make_async_copy(diag, weights.at[0], load_sem.at[1]),
        pltpu.make_async_copy(coupling.at[0], slots, load_sem.at[2]),
        pltpu.make_async_copy(trial, roots.at[z], load_sem.at[3]),
        pltpu.make_async_copy(partners_in, partners, load_sem.at[4]),
        pltpu.make_async_copy(beta_in, beta, load_sem.at[5]),
        pltpu.make_async_copy(hdiag_in, hdiag, load_sem.at[6]),
    ]
    for load in loads:
        load.start()

    barrier = pltpu.get_barrier_semaphore()
    for r in range(1, members):
        pl.semaphore_signal(barrier, inc=1, device_id={"blk": peer(r)}, device_id_type=MESH)

    @pl.when(z < depth - 1)
    def _():
        pl.semaphore_signal(barrier, inc=1, device_id={"vec": z + 1}, device_id_type=MESH)

    @pl.when(z > 0)
    def _():
        pl.semaphore_signal(barrier, inc=1, device_id={"vec": z - 1}, device_id_type=MESH)

    pl.semaphore_wait(barrier, members + 1 - is_end.astype(jnp.int32))

    def blk_copy(r, hop, c):
        src = trial if r == 0 else held.at[r]
        return remote(
            part(src, c), part(held.at[r ^ hop], c), blk_send.at[r ^ hop, c], blk_recv.at[r ^ hop, c],
            {"blk": peer(hop)},
        )

    sent = []

    def blk_start(r, hop, c):
        copy = blk_copy(r, hop, c)
        copy.start()
        sent.append(copy)

    def blk_wait(slot, c):
        blk_copy(0, slot, c).wait_recv()

    def vec_copy(origin, side, c, src):
        return remote(
            part(src, c), part(roots.at[origin], c), vec_send.at[side, origin, c], vec_recv.at[origin, c],
            {"vec": z + 1 - 2 * side},
        )

    def goes(side, c):
        limit = 2 if c == last else 1
        return (z < depth - limit) if side == 0 else (z >= limit)

    def has(step, side, c):
        origin = z - step if side == 0 else z + step
        there = (origin >= 0) & (origin < depth)
        if c == last:
            there = there & jnp.logical_not(is_end)
        return there, origin

    for c in range(CHUNKS):
        blk_start(0, 2, c)
        blk_start(0, 4, (c + 2) % CHUNKS)
        blk_start(0, 1, c)
        for side in (0, 1):
            @pl.when(goes(side, c))
            def _():
                vec_copy(z, side, c, trial).start()

    def vec_step(step, c):
        for side in (0, 1):
            there, origin = has(step, side, c)

            @pl.when(there)
            def _():
                vec_copy(origin, side, c, trial).wait_recv()

            @pl.when(there & goes(side, c))
            def _():
                vec_copy(origin, side, c, roots.at[origin]).start()

    for load in loads:
        load.wait()

    def select(r):
        block = peer(r)
        index, hit = jnp.int32(0), jnp.float32(0.0)
        for c in range(slots.shape[0]):
            match = (partners[0, c] == block) & (c < live[0])
            index = jnp.where(match, c, index)
            hit = jnp.where(match, jnp.float32(1.0), hit)
        weights[r] = (slots[index].astype(jnp.float32) * hit).astype(weights.dtype)

    for r in range(1, members):
        select(r)

    def own(k, _):
        vectors = held[0, k]
        sigma[k] = (
            jnp.dot(beta[...], vectors, preferred_element_type=jnp.float32)
            + hdiag[...] * vectors.astype(jnp.float32)
        )
        return 0

    lax.fori_loop(0, root_count, own, 0)

    def multiply(r, c):
        span = pl.ds(pl.multiple_of(c * piece, piece), piece)
        left = held[r, :, span, :].reshape(cells, width)
        out = lax.dot_general(left, weights[r], CONTRACT, preferred_element_type=jnp.float32)
        sigma[:, span, :] += out.reshape(root_count, piece, width)

    def multiply_all(first, count):
        def body(i, _):
            multiply(first + i // CHUNKS, i % CHUNKS)
            return 0

        lax.fori_loop(0, count * CHUNKS, body, 0)

    for c in range(CHUNKS):
        blk_wait(1, c)
    multiply_all(0, 2)
    products[...] = jnp.zeros_like(products)

    for t in range(CHUNKS):
        u = (t + 2) % CHUNKS
        blk_wait(2, t)
        if t < 2:
            blk_start(2, 4, t)
        blk_start(2, 1, t)
        blk_wait(4, u)
        if t < 2:
            blk_start(4, 2, u)
        blk_start(4, 1, u)
        vec_step(1, t)
    for c in range(CHUNKS):
        blk_wait(3, c)
        blk_wait(5, c)
    multiply_all(2, 4)
    for t in range(2):
        for c in (t, t + 2):
            blk_wait(6, c)
            blk_start(6, 1, c)
        vec_step(2, t)
        for c in (t, t + 2):
            blk_wait(7, c)

        def tail(i, _, t=t):
            multiply(6 + i // 2, t + 2 * (i % 2))
            return 0

        lax.fori_loop(0, 4, tail, 0)

    def share(phase):
        for r in range(1, members):
            place = stats.at[phase, me]
            remote(place, place, stat_send.at[phase, r], stat_recv.at[phase, me], {"blk": peer(r)}).start()

    def gather(phase):
        for r in range(1, members):
            place = stats.at[phase, peer(r)]
            remote(place, place, stat_send.at[phase, r], stat_recv.at[phase, peer(r)], {"blk": peer(r)}).wait_recv()
        total = stats[phase, 0]
        for j in range(1, members):
            total = total + stats[phase, j]
        return total

    def finish(k, _):
        value = sigma[k]
        rounded[k] = value.astype(rounded.dtype)
        rows[pl.ds(k, 1), :] = jnp.sum(value * held[0, k].astype(jnp.float32), axis=0, keepdims=True)
        return 0

    lax.fori_loop(0, root_count, finish, 0)
    stats[0, me] = jnp.broadcast_to(jnp.sum(rows[...], axis=1, keepdims=True), stats.shape[2:])
    share(0)

    def edge_copy():
        return remote(part(rounded, last), edge, edge_send.at[0], edge_recv.at[0], {"vec": mate})

    def total_copy():
        return remote(edge_total.at[0], edge_total.at[1], edge_send.at[1], edge_recv.at[1], {"vec": mate})

    @pl.when(is_end)
    def _():
        edge_copy().start()

    row = lax.broadcasted_iota(jnp.int32, (cells, cells), 0) % piece
    column = lax.broadcasted_iota(jnp.int32, (cells, cells), 1) % piece
    same = (row == column).astype(jnp.float32)

    def product(which, origin, c, right):
        span = pl.ds(pl.multiple_of(c * piece, piece), piece)
        left = roots[origin, :, span, :].reshape(cells, width)
        out = lax.dot_general(left, right.reshape(cells, width), CONTRACT, preferred_element_type=jnp.float32)
        out = jnp.sum((out * same).reshape(root_count, piece, cells), axis=1)
        place = pl.ds(pl.multiple_of(origin * root_count, root_count), root_count)
        products[which, place, :] += out

    def products_of(origin, start, stop):
        def body(c, _):
            span = pl.ds(pl.multiple_of(c * piece, piece), piece)
            product(0, origin, c, rounded[:, span, :])
            return 0

        lax.fori_loop(start, stop, body, 0)

    def products_at(step, start, stop):
        for side in (0, 1):
            for low, high in ((start, min(stop, last)), (max(start, last), stop)):
                if low < high:
                    there, origin = has(step, side, low)

                    @pl.when(there)
                    def _():
                        products_of(origin, low, high)

    products_of(z, 0, last)

    @pl.when(jnp.logical_not(is_end))
    def _():
        products_of(z, last, CHUNKS)

    products_at(1, 0, CHUNKS)
    vec_step(2, 2)
    products_at(2, 0, last)

    theta[...] = jnp.broadcast_to(gather(0)[:, :1], theta.shape)

    def residual(k, _):
        value = theta[pl.ds(k, 1), :]
        resid = sigma[k] - value * held[0, k].astype(jnp.float32)
        gap = value - hdiag[...]
        raw = resid * gap / (gap * gap + 0.25)
        sigma[k] = raw
        rows[pl.ds(k, 1), :] = jnp.sum(raw * raw, axis=0, keepdims=True)
        return 0

    lax.fori_loop(0, root_count, residual, 0)
    stats[1, me] = jnp.broadcast_to(jnp.sum(rows[...], axis=1, keepdims=True), stats.shape[2:])
    share(1)
    msq = gather(1) / (beta_count * width * members)
    theta[...] = jnp.broadcast_to(lax.rsqrt(msq + 1e-06)[:, :1], theta.shape)

    def scale(k, _):
        correction[k] = (sigma[k] * theta[pl.ds(k, 1), :]).astype(correction.dtype)
        return 0

    lax.fori_loop(0, root_count, scale, 0)

    pick = (
        lax.broadcasted_iota(jnp.int32, (root_count, cells), 1) // piece
        == lax.broadcasted_iota(jnp.int32, (root_count, cells), 0)
    ).astype(jnp.float32)

    def collect(which):
        return lax.dot_general(
            pick, products[which], CONTRACT, precision=lax.Precision.HIGHEST, preferred_element_type=jnp.float32
        )

    vec_step(2, last)
    products_at(2, last, CHUNKS)

    @pl.when(jnp.logical_not(is_end))
    def _():
        edge_copy().wait_recv()

        def body(origin, _):
            product(1, origin, last, edge[...])
            return 0

        lax.fori_loop(0, depth, body, 0)
        edge_total[0] = collect(1)
        total_copy().start()

    for c in range(last):
        vec_step(3, c)
        products_at(3, c, c + 1)
    totals[...] = collect(0)

    @pl.when(is_end)
    def _():
        total_copy().wait_recv()
        totals[...] += edge_total[1]

    stats[2, me] = totals[...]
    share(2)

    for copy in sent:
        copy.wait_send()
    for side in (0, 1):
        for c in range(CHUNKS):
            @pl.when(goes(side, c))
            def _():
                vec_copy(z, side, c, trial).wait_send()

            for step in range(1, depth):
                there, origin = has(step, side, c)

                @pl.when(there & goes(side, c))
                def _():
                    vec_copy(origin, side, c, trial).wait_send()

    @pl.when(is_end)
    def _():
        edge_copy().wait_send()

    @pl.when(jnp.logical_not(is_end))
    def _():
        total_copy().wait_send()

    subspace[...] = gather(2)
    for phase in range(3):
        for r in range(1, members):
            place = stats.at[phase, me]
            remote(place, place, stat_send.at[phase, r], stat_recv.at[phase, me], {"blk": peer(r)}).wait_send()


def exchanged(depth, members, trial, coupling, partners, live, diag_block, beta_coupling, hdiag):
    root_count, beta_count, width = trial.shape
    slot_count = coupling.shape[1]
    cells = root_count * (beta_count // CHUNKS)
    lanes = 128
    kind, full = trial.dtype, jnp.float32
    vmem, smem, anywhere = (
        pl.BlockSpec(memory_space=pltpu.VMEM),
        pl.BlockSpec(memory_space=pltpu.SMEM),
        pl.BlockSpec(memory_space=pltpu.HBM),
    )
    dma = pltpu.SemaphoreType.DMA
    correction, subspace = pl.pallas_call(
        functools.partial(kernel, depth),
        out_shape=(
            jax.ShapeDtypeStruct(trial.shape, kind),
            jax.ShapeDtypeStruct((root_count, lanes), full),
        ),
        in_specs=[anywhere, smem] + [anywhere] * 5,
        out_specs=(vmem, vmem),
        scratch_shapes=[
            pltpu.SMEM(partners.shape, partners.dtype),
            pltpu.VMEM(beta_coupling.shape, beta_coupling.dtype),
            pltpu.VMEM(hdiag.shape, hdiag.dtype),
            pltpu.VMEM((members,) + trial.shape, kind),
            pltpu.VMEM((members, width, width), kind),
            pltpu.VMEM((slot_count, width, width), kind),
            pltpu.VMEM((depth,) + trial.shape, kind),
            pltpu.VMEM(trial.shape, full),
            pltpu.VMEM(trial.shape, kind),
            pltpu.VMEM((root_count, beta_count // CHUNKS, width), kind),
            pltpu.VMEM((root_count, width), full),
            pltpu.VMEM((3, members, root_count, lanes), full),
            pltpu.VMEM((2, lanes, cells), full),
            pltpu.VMEM((root_count, width), full),
            pltpu.VMEM((root_count, lanes), full),
            pltpu.VMEM((2, root_count, lanes), full),
            dma((7,)),
            dma((members, CHUNKS)),
            dma((members, CHUNKS)),
            dma((2, depth, CHUNKS)),
            dma((depth, CHUNKS)),
            dma((3, members)),
            dma((3, members)),
            dma((2,)),
            dma((2,)),
        ],
        compiler_params=pltpu.CompilerParams(collective_id=0, has_side_effects=True, vmem_limit_bytes=50 * 2**20),
        name="davidson",
    )(partners, live, trial, coupling, diag_block, beta_coupling, hdiag)
    return correction, subspace[:, : root_count * depth].T


def solution(mesh):
    depth, members = mesh.shape["vec"], mesh.shape["blk"]
    if depth == 4 and members == 8:
        local = functools.partial(exchanged, depth, members)
    else:
        local = gathered
    in_specs = (
        P("vec", None, "blk"),
        P("blk", None, None, None),
        P("blk", None),
        P("blk"),
        P("blk", None),
        P(),
        P(None, "blk"),
    )
    out_specs = (P("vec", None, "blk"), P(None, "vec"))
    return jax.shard_map(local, mesh=mesh, in_specs=in_specs, out_specs=out_specs, check_vma=False)
```

```python
import functools

import jax
import jax.numpy as jnp
from jax import lax
from jax.experimental import pallas as pl
from jax.experimental.pallas import tpu as pltpu
from jax.sharding import PartitionSpec as P


def gathered(trial, coupling, partners, live, diag_block, beta_coupling, hdiag):
    root_count, beta_count, block_width = trial.shape
    row_count = root_count * beta_count
    contract = (((1,), (1,)), ((), ()))
    blocks = coupling[0]
    partner_ids = partners[0]
    live_count = live[0]
    flat = trial.reshape(row_count, block_width)
    sigma_flat = lax.dot_general(flat, diag_block, contract, preferred_element_type=jnp.float32)
    empty = jnp.zeros((row_count, block_width), jnp.float32)
    running = empty
    segment = lax.all_gather(trial, "blk", axis=2, tiled=True)
    span_width = segment.shape[2]
    seg_flat = segment.reshape(row_count, span_width)
    for member in range(blocks.shape[0]):
        relative = partner_ids[member] * block_width
        inside = (relative >= 0) & (relative + block_width <= span_width) & (member < live_count)
        start = jnp.clip(relative, 0, span_width - block_width)

        def multiply(total, start=start, member=member):
            piece = lax.dynamic_slice_in_dim(seg_flat, start, block_width, 1)
            return total + lax.dot_general(
                piece, blocks[member], contract, preferred_element_type=jnp.float32
            )

        def unchanged(total):
            return total

        running = lax.cond(inside, multiply, unchanged, running)
    trial_float = trial.astype(jnp.float32)
    beta_part = jnp.einsum("bc,kca->kba", beta_coupling, trial, preferred_element_type=jnp.float32)
    sigma = (
        (sigma_flat + running).reshape(root_count, beta_count, block_width)
        + beta_part
        + hdiag[None] * trial_float
    )
    all_roots = lax.all_gather(trial, "vec", axis=0, tiled=True)
    intersection_part = jnp.einsum(
        "kba,lba->kl", all_roots.astype(jnp.float32), sigma, precision=lax.Precision.HIGHEST
    )
    total_cells = beta_count * block_width * lax.axis_size("blk")
    theta_part = jnp.einsum("kba,kba->k", trial_float, sigma, precision=lax.Precision.HIGHEST)
    theta = lax.psum(theta_part, "blk")
    resid = sigma - theta[:, None, None] * trial_float
    gap = theta[:, None, None] - hdiag[None]
    raw = resid * gap / (gap * gap + 0.25)
    squares, subspace = lax.psum((jnp.sum(raw * raw, axis=(1, 2)), intersection_part), "blk")
    msq = squares / total_cells
    correction = (raw * lax.rsqrt(msq + 1e-06)[:, None, None]).astype(jnp.bfloat16)
    return (correction, subspace)


CHUNKS = 4
MESH = pl.DeviceIdType.MESH
CONTRACT = (((1,), (1,)), ((), ()))


def kernel(
    depth, partners_in, live, trial, coupling, diag, beta_in, hdiag_in, correction, subspace,
    partners, beta, hdiag, held, weights, slots, roots, sigma, rounded, edge, rows, stats, products, theta, totals, edge_total,
    load_sem, blk_send, blk_recv, vec_send, vec_recv, stat_send, stat_recv, edge_send, edge_recv,
):
    me, z = lax.axis_index("blk"), lax.axis_index("vec")
    root_count, beta_count, width = trial.shape
    piece = beta_count // CHUNKS
    cells = root_count * piece
    last = CHUNKS - 1
    members = held.shape[0]
    core, x, y = me % 2, (me // 2) % 2, me // 4
    is_end = (z == 0) | (z == depth - 1)
    mate = z + 1 - 2 * (z % 2)

    def peer(r):
        flip = lambda bit, on: 1 - bit if on else bit
        return flip(y, r & 4) * 4 + flip(x, r & 2) * 2 + flip(core, r & 1)

    def part(ref, c):
        return ref.at[:, pl.ds(c * piece, piece), :]

    def remote(src, dst, send, recv, device):
        return pltpu.make_async_remote_copy(
            src_ref=src, dst_ref=dst, send_sem=send, recv_sem=recv, device_id=device, device_id_type=MESH
        )

    loads = [
        pltpu.make_async_copy(trial, held.at[0], load_sem.at[0]),
        pltpu.make_async_copy(diag, weights.at[0], load_sem.at[1]),
        pltpu.make_async_copy(coupling.at[0], slots, load_sem.at[2]),
        pltpu.make_async_copy(trial, roots.at[z], load_sem.at[3]),
        pltpu.make_async_copy(partners_in, partners, load_sem.at[4]),
        pltpu.make_async_copy(beta_in, beta, load_sem.at[5]),
        pltpu.make_async_copy(hdiag_in, hdiag, load_sem.at[6]),
    ]
    for load in loads:
        load.start()

    barrier = pltpu.get_barrier_semaphore()
    for r in range(1, members):
        pl.semaphore_signal(barrier, inc=1, device_id={"blk": peer(r)}, device_id_type=MESH)

    @pl.when(z < depth - 1)
    def _():
        pl.semaphore_signal(barrier, inc=1, device_id={"vec": z + 1}, device_id_type=MESH)

    @pl.when(z > 0)
    def _():
        pl.semaphore_signal(barrier, inc=1, device_id={"vec": z - 1}, device_id_type=MESH)

    pl.semaphore_wait(barrier, members + 1 - is_end.astype(jnp.int32))

    def blk_copy(r, hop, c):
        src = trial if r == 0 else held.at[r]
        return remote(
            part(src, c), part(held.at[r ^ hop], c), blk_send.at[r ^ hop, c], blk_recv.at[r ^ hop, c],
            {"blk": peer(hop)},
        )

    sent = []

    def blk_start(r, hop, c):
        copy = blk_copy(r, hop, c)
        copy.start()
        sent.append(copy)

    def blk_wait(slot, c):
        blk_copy(0, slot, c).wait_recv()

    def vec_copy(origin, side, c, src):
        return remote(
            part(src, c), part(roots.at[origin], c), vec_send.at[side, origin, c], vec_recv.at[origin, c],
            {"vec": z + 1 - 2 * side},
        )

    def goes(side, c):
        limit = 2 if c == last else 1
        return (z < depth - limit) if side == 0 else (z >= limit)

    def has(step, side, c):
        origin = z - step if side == 0 else z + step
        there = (origin >= 0) & (origin < depth)
        if c == last:
            there = there & jnp.logical_not(is_end)
        return there, origin

    for c in range(CHUNKS):
        blk_start(0, 2, c)
        blk_start(0, 4, (c + 2) % CHUNKS)
        blk_start(0, 1, c)
        for side in (0, 1):
            @pl.when(goes(side, c))
            def _():
                vec_copy(z, side, c, trial).start()

    def vec_step(step, c):
        for side in (0, 1):
            there, origin = has(step, side, c)

            @pl.when(there)
            def _():
                vec_copy(origin, side, c, trial).wait_recv()

            @pl.when(there & goes(side, c))
            def _():
                vec_copy(origin, side, c, roots.at[origin]).start()

    for load in loads:
        load.wait()

    def select(r):
        block = peer(r)
        index, hit = jnp.int32(0), jnp.float32(0.0)
        for c in range(slots.shape[0]):
            match = (partners[0, c] == block) & (c < live[0])
            index = jnp.where(match, c, index)
            hit = jnp.where(match, jnp.float32(1.0), hit)
        weights[r] = (slots[index].astype(jnp.float32) * hit).astype(weights.dtype)

    for r in range(1, members):
        select(r)

    def own(k, _):
        vectors = held[0, k]
        sigma[k] = (
            jnp.dot(beta[...], vectors, preferred_element_type=jnp.float32)
            + hdiag[...] * vectors.astype(jnp.float32)
        )
        return 0

    lax.fori_loop(0, root_count, own, 0)

    def multiply(r, c):
        span = pl.ds(pl.multiple_of(c * piece, piece), piece)
        left = held[r, :, span, :].reshape(cells, width)
        out = lax.dot_general(left, weights[r], CONTRACT, preferred_element_type=jnp.float32)
        sigma[:, span, :] += out.reshape(root_count, piece, width)

    def multiply_all(first, count):
        def body(i, _):
            multiply(first + i // CHUNKS, i % CHUNKS)
            return 0

        lax.fori_loop(0, count * CHUNKS, body, 0)

    for c in range(CHUNKS):
        blk_wait(1, c)
    multiply_all(0, 2)
    products[...] = jnp.zeros_like(products)

    for t in range(CHUNKS):
        u = (t + 2) % CHUNKS
        blk_wait(2, t)
        if t < 2:
            blk_start(2, 4, t)
        blk_start(2, 1, t)
        blk_wait(4, u)
        if t < 2:
            blk_start(4, 2, u)
        blk_start(4, 1, u)
        vec_step(1, t)
    for c in range(CHUNKS):
        blk_wait(3, c)
        blk_wait(5, c)
    multiply_all(2, 4)
    for t in range(2):
        for c in (t, t + 2):
            blk_wait(6, c)
            blk_start(6, 1, c)
        vec_step(2, t)
        for c in (t, t + 2):
            blk_wait(7, c)

        def tail(i, _, t=t):
            multiply(6 + i // 2, t + 2 * (i % 2))
            return 0

        lax.fori_loop(0, 4, tail, 0)

    def share(phase):
        for r in range(1, members):
            place = stats.at[phase, me]
            remote(place, place, stat_send.at[phase, r], stat_recv.at[phase, me], {"blk": peer(r)}).start()

    def gather(phase):
        for r in range(1, members):
            place = stats.at[phase, peer(r)]
            remote(place, place, stat_send.at[phase, r], stat_recv.at[phase, peer(r)], {"blk": peer(r)}).wait_recv()
        total = stats[phase, 0]
        for j in range(1, members):
            total = total + stats[phase, j]
        return total

    def finish(k, _):
        value = sigma[k]
        rounded[k] = value.astype(rounded.dtype)
        rows[pl.ds(k, 1), :] = jnp.sum(value * held[0, k].astype(jnp.float32), axis=0, keepdims=True)
        return 0

    lax.fori_loop(0, root_count, finish, 0)
    stats[0, me] = jnp.broadcast_to(jnp.sum(rows[...], axis=1, keepdims=True), stats.shape[2:])
    share(0)

    def edge_copy():
        return remote(part(rounded, last), edge, edge_send.at[0], edge_recv.at[0], {"vec": mate})

    def total_copy():
        return remote(edge_total.at[0], edge_total.at[1], edge_send.at[1], edge_recv.at[1], {"vec": mate})

    @pl.when(is_end)
    def _():
        edge_copy().start()

    row = lax.broadcasted_iota(jnp.int32, (cells, cells), 0) % piece
    column = lax.broadcasted_iota(jnp.int32, (cells, cells), 1) % piece
    same = (row == column).astype(jnp.float32)

    def product(which, origin, c, right):
        span = pl.ds(pl.multiple_of(c * piece, piece), piece)
        left = roots[origin, :, span, :].reshape(cells, width)
        out = lax.dot_general(left, right.reshape(cells, width), CONTRACT, preferred_element_type=jnp.float32)
        out = jnp.sum((out * same).reshape(root_count, piece, cells), axis=1)
        place = pl.ds(pl.multiple_of(origin * root_count, root_count), root_count)
        products[which, place, :] += out

    def products_of(origin, start, stop):
        def body(c, _):
            span = pl.ds(pl.multiple_of(c * piece, piece), piece)
            product(0, origin, c, rounded[:, span, :])
            return 0

        lax.fori_loop(start, stop, body, 0)

    def products_at(step, start, stop):
        for side in (0, 1):
            for low, high in ((start, min(stop, last)), (max(start, last), stop)):
                if low < high:
                    there, origin = has(step, side, low)

                    @pl.when(there)
                    def _():
                        products_of(origin, low, high)

    products_of(z, 0, last)

    @pl.when(jnp.logical_not(is_end))
    def _():
        products_of(z, last, CHUNKS)

    products_at(1, 0, CHUNKS)
    vec_step(2, 2)
    products_at(2, 0, last)

    theta[...] = jnp.broadcast_to(gather(0)[:, :1], theta.shape)

    def residual(k, _):
        value = theta[pl.ds(k, 1), :]
        resid = sigma[k] - value * held[0, k].astype(jnp.float32)
        gap = value - hdiag[...]
        raw = resid * gap / (gap * gap + 0.25)
        sigma[k] = raw
        rows[pl.ds(k, 1), :] = jnp.sum(raw * raw, axis=0, keepdims=True)
        return 0

    lax.fori_loop(0, root_count, residual, 0)
    stats[1, me] = jnp.broadcast_to(jnp.sum(rows[...], axis=1, keepdims=True), stats.shape[2:])
    share(1)
    msq = gather(1) / (beta_count * width * members)
    theta[...] = jnp.broadcast_to(lax.rsqrt(msq + 1e-06)[:, :1], theta.shape)

    def scale(k, _):
        correction[k] = (sigma[k] * theta[pl.ds(k, 1), :]).astype(correction.dtype)
        return 0

    lax.fori_loop(0, root_count, scale, 0)

    pick = (
        lax.broadcasted_iota(jnp.int32, (root_count, cells), 1) // piece
        == lax.broadcasted_iota(jnp.int32, (root_count, cells), 0)
    ).astype(jnp.float32)

    def collect(which):
        return lax.dot_general(
            pick, products[which], CONTRACT, precision=lax.Precision.HIGHEST, preferred_element_type=jnp.float32
        )

    vec_step(2, last)
    products_at(2, last, CHUNKS)

    @pl.when(jnp.logical_not(is_end))
    def _():
        edge_copy().wait_recv()

        def body(origin, _):
            product(1, origin, last, edge[...])
            return 0

        lax.fori_loop(0, depth, body, 0)
        edge_total[0] = collect(1)
        total_copy().start()

    for c in range(last):
        vec_step(3, c)
        products_at(3, c, c + 1)
    totals[...] = collect(0)

    @pl.when(is_end)
    def _():
        total_copy().wait_recv()
        totals[...] += edge_total[1]

    stats[2, me] = totals[...]
    share(2)

    for copy in sent:
        copy.wait_send()
    for side in (0, 1):
        for c in range(CHUNKS):
            @pl.when(goes(side, c))
            def _():
                vec_copy(z, side, c, trial).wait_send()

            for step in range(1, depth):
                there, origin = has(step, side, c)

                @pl.when(there & goes(side, c))
                def _():
                    vec_copy(origin, side, c, trial).wait_send()

    @pl.when(is_end)
    def _():
        edge_copy().wait_send()

    @pl.when(jnp.logical_not(is_end))
    def _():
        total_copy().wait_send()

    subspace[...] = gather(2)
    for phase in range(3):
        for r in range(1, members):
            place = stats.at[phase, me]
            remote(place, place, stat_send.at[phase, r], stat_recv.at[phase, me], {"blk": peer(r)}).wait_send()


def exchanged(depth, members, trial, coupling, partners, live, diag_block, beta_coupling, hdiag):
    root_count, beta_count, width = trial.shape
    slot_count = coupling.shape[1]
    cells = root_count * (beta_count // CHUNKS)
    lanes = 128
    kind, full = trial.dtype, jnp.float32
    vmem, smem, anywhere = (
        pl.BlockSpec(memory_space=pltpu.VMEM),
        pl.BlockSpec(memory_space=pltpu.SMEM),
        pl.BlockSpec(memory_space=pltpu.HBM),
    )
    dma = pltpu.SemaphoreType.DMA
    correction, subspace = pl.pallas_call(
        functools.partial(kernel, depth),
        out_shape=(
            jax.ShapeDtypeStruct(trial.shape, kind),
            jax.ShapeDtypeStruct((root_count, lanes), full),
        ),
        in_specs=[anywhere, smem] + [anywhere] * 5,
        out_specs=(vmem, vmem),
        scratch_shapes=[
            pltpu.SMEM(partners.shape, partners.dtype),
            pltpu.VMEM(beta_coupling.shape, beta_coupling.dtype),
            pltpu.VMEM(hdiag.shape, hdiag.dtype),
            pltpu.VMEM((members,) + trial.shape, kind),
            pltpu.VMEM((members, width, width), kind),
            pltpu.VMEM((slot_count, width, width), kind),
            pltpu.VMEM((depth,) + trial.shape, kind),
            pltpu.VMEM(trial.shape, full),
            pltpu.VMEM(trial.shape, kind),
            pltpu.VMEM((root_count, beta_count // CHUNKS, width), kind),
            pltpu.VMEM((root_count, width), full),
            pltpu.VMEM((3, members, root_count, lanes), full),
            pltpu.VMEM((2, lanes, cells), full),
            pltpu.VMEM((root_count, width), full),
            pltpu.VMEM((root_count, lanes), full),
            pltpu.VMEM((2, root_count, lanes), full),
            dma((7,)),
            dma((members, CHUNKS)),
            dma((members, CHUNKS)),
            dma((2, depth, CHUNKS)),
            dma((depth, CHUNKS)),
            dma((3, members)),
            dma((3, members)),
            dma((2,)),
            dma((2,)),
        ],
        compiler_params=pltpu.CompilerParams(collective_id=0, has_side_effects=True),
        name="davidson",
    )(partners, live, trial, coupling, diag_block, beta_coupling, hdiag)
    return correction, subspace[:, : root_count * depth].T


def solution(mesh):
    depth, members = mesh.shape["vec"], mesh.shape["blk"]
    if depth == 4 and members == 8:
        local = functools.partial(exchanged, depth, members)
    else:
        local = gathered
    in_specs = (
        P("vec", None, "blk"),
        P("blk", None, None, None),
        P("blk", None),
        P("blk"),
        P("blk", None),
        P(),
        P(None, "blk"),
    )
    out_specs = (P("vec", None, "blk"), P(None, "vec"))
    return jax.shard_map(local, mesh=mesh, in_specs=in_specs, out_specs=out_specs, check_vma=False)
```
